32 devices in a mesh: ka: 8 (over z, x), row: 4 (over y, core).
Axes of the slice: x: 2, y: 2, z: 4, core: 2. Of those that a mesh axis runs over, the one named last changes fastest.
Arguments:
- gauge: bfloat16 [32, 2, 384, 384], P(('ka', 'row')), may hold values from -3 to 3
- energies: float32 [32, 384], P(('ka', 'row')), may hold values from -5 to 5
- kmesh: int32 [3, 32], replicated, may hold values from 0 to 11
- lattice: int32 [3, 256], P(None, 'row'), may hold values from -8 to 8
- degeneracy: int32 [256], P('row'), may hold values from 1 to 8
- path: int32 [3, 8], replicated, may hold values from 0 to 63
Outputs:
- lattice_h: bfloat16 [256, 384, 768], P('row', 'ka')
- path_h: float32 [8, 384, 768], P('row', 'ka')
The draws below stay inside these ranges and needn't reach their ends.
All inputs are finite; a program needn't handle non-finite values.
Results may differ from the reference program's by a relative error of at most 0.006.
Values may be sent and summed in bfloat16 or wider, within the bound.
No kernel may reach another device: no remote copies, remote signals or barrier semaphores. Data moves between devices by JAX's collectives and lax.ppermute only.
A program may use at most 64 MiB of HBM per device.

```python
import math
import jax
import jax.numpy as jnp
from jax import lax

W = 384
MESH = 12
PATH_DEN = 64
R_DEV = 64
NK = 32
NR = 256
NP = 8
N_ROW = 4


def plant(result, rng, least, top_value):
    index_at = [jax.random.randint(jax.random.fold_in(rng, axis), (), 0, length) for axis, length in enumerate(result.shape)]
    widest = result.shape.index(max(result.shape))
    beside = index_at[:widest] + [(index_at[widest] + 1) % result.shape[widest]] + index_at[widest + 1:]
    return result.at[tuple(index_at)].set(least).at[tuple(beside)].set(top_value)


def block_levels(rng, extent, split, low, high):
    def one(position, shards_of):
        steps = jax.random.uniform(jax.random.fold_in(jax.random.fold_in(rng, 6), position), (shards_of,), jnp.float32, low / len(split), high / len(split))
        return jnp.repeat(jnp.exp(steps), extent[position] // shards_of).reshape((-1,) + (1,) * (len(extent) - position - 1))

    loudness = one(*split[0])
    for cut in split[1:]:
        loudness = loudness * one(*cut)
    return loudness


def bell_draw(own_key, shape, deviation, reach, pieces=(), held_as=jnp.bfloat16):
    array = jax.random.normal(own_key, shape, jnp.float32) * deviation
    if len(pieces) > 0:
        array = block_levels(own_key, shape, pieces, -0.22, 0.18) * array
    return jnp.clip(array, min=-reach, max=reach).astype(held_as)


def setup_inputs(seed: int = 0) -> dict:
    arg_keys = jax.random.split(jax.random.key(seed), 7)
    return {
        "gauge": bell_draw(arg_keys[0], (NK, 2, W, W), 0.5, 3.0, ((0, 32),)),
        "energies": bell_draw(arg_keys[1], (NK, W), 1.0, 5.0, ((0, 32),), jnp.float32),
        "kmesh": plant(jax.random.randint(arg_keys[2], (3, NK), 0, MESH), jax.random.fold_in(arg_keys[2], 1), 0, MESH - 1).astype(jnp.int32),
        "lattice": plant(jax.random.randint(arg_keys[3], (3, NR), -8, 9), jax.random.fold_in(arg_keys[3], 1), -8, 8).astype(jnp.int32),
        "degeneracy": plant(jax.random.randint(arg_keys[4], (NR,), 1, 9), jax.random.fold_in(arg_keys[4], 1), 1, 8).astype(jnp.int32),
        "path": plant(jax.random.randint(arg_keys[5], (3, NP), 0, PATH_DEN), jax.random.fold_in(arg_keys[5], 1), 0, PATH_DEN - 1).astype(jnp.int32),
    }


def rotate(pair):
    gauge_one, energy_one = pair
    scaled = (energy_one[None, :, None] * gauge_one.astype(jnp.float32)).astype(jnp.bfloat16)
    scaled_re = scaled[0].astype(jnp.float32)
    scaled_im = scaled[1].astype(jnp.float32)
    stacked = jnp.concatenate([gauge_one[0], gauge_one[1]], 0).astype(jnp.float32)
    partner = jnp.concatenate([jnp.concatenate([scaled_re, scaled_im], 1), jnp.concatenate([scaled_im, -scaled_re], 1)], 0)
    return jnp.dot(stacked.T, partner, preferred_element_type=jnp.float32).astype(jnp.bfloat16)


def reference(gauge, energies, kmesh, lattice, degeneracy, path):
    k_total = kmesh.shape[1]
    orbitals = gauge.shape[2]
    path_total = path.shape[1]
    rotated = lax.map(rotate, (gauge, energies))
    flattened = rotated.reshape(k_total, -1).astype(jnp.float32)
    vector_blocks = lattice.reshape(3, N_ROW, R_DEV).transpose(1, 0, 2)
    multiples = degeneracy.reshape(N_ROW, R_DEV)

    def step_block(running, block_in):
        vectors, counts_r = block_in
        windings = jnp.mod(jnp.sum(vectors[:, :, None] * kmesh[:, None, :], 0), MESH).astype(jnp.int32)
        angles = windings.astype(jnp.float32) * (2.0 * math.pi / MESH)
        factors = jnp.concatenate([jnp.cos(angles), jnp.sin(angles)], 0).astype(jnp.bfloat16)
        factors = lax.optimization_barrier(factors).astype(jnp.float32)
        products = jnp.dot(factors, flattened, preferred_element_type=jnp.float32)
        products = products.reshape(2, R_DEV, orbitals, 2, orbitals)
        real_part = products[0, :, :, 0] + products[1, :, :, 1]
        imag_part = products[0, :, :, 1] - products[1, :, :, 0]
        lattice_f = jnp.concatenate([real_part, imag_part], -1) / k_total
        windings_p = jnp.mod(jnp.sum(path[:, :, None] * vectors[:, None, :], 0), PATH_DEN).astype(jnp.int32)
        angles_p = windings_p.astype(jnp.float32) * (2.0 * math.pi / PATH_DEN)
        weights = 1.0 / counts_r.astype(jnp.float32)
        factors_p = jnp.concatenate([jnp.cos(angles_p) * weights[None, :], jnp.sin(angles_p) * weights[None, :]], 0).astype(jnp.bfloat16)
        factors_p = lax.optimization_barrier(factors_p).astype(jnp.float32)
        values = jnp.dot(factors_p, lattice_f.reshape(R_DEV, -1), preferred_element_type=jnp.float32)
        values = values.reshape(2, path_total, orbitals, 2, orbitals)
        real_p = values[0, :, :, 0] - values[1, :, :, 1]
        imag_p = values[0, :, :, 1] + values[1, :, :, 0]
        return running + jnp.concatenate([real_p, imag_p], -1), lattice_f.astype(jnp.bfloat16)

    initial = jnp.zeros((path_total, orbitals, 2 * orbitals), jnp.float32)
    path_h, blocks = lax.scan(step_block, initial, (vector_blocks, multiples))
    lattice_h = blocks.reshape(N_ROW * R_DEV, orbitals, 2 * orbitals)
    return lattice_h, path_h
```

```python
import functools
import math

import jax
import jax.numpy as jnp
from jax import lax
from jax.experimental import pallas as pl
from jax.experimental.pallas import tpu as pltpu
from jax.sharding import PartitionSpec as P

MESH = 12
PATH_DEN = 64
SUB = 8


def rotate_kernel(gauge_ref, energy_ref, out_ref):
    orbitals = gauge_ref.shape[-1]
    bands = gauge_ref.shape[-2]
    for k in range(gauge_ref.shape[0]):
        energy = jnp.broadcast_to(energy_ref[k : k + 1, :], (SUB, bands)).T[:, :1]
        ur, ui = gauge_ref[k, 0], gauge_ref[k, 1]
        sr = (energy * ur.astype(jnp.float32)).astype(jnp.bfloat16)
        si = (energy * ui.astype(jnp.float32)).astype(jnp.bfloat16)
        contract = lambda a, b: lax.dot_general(
            a, b, (((0,), (0,)), ((), ())), preferred_element_type=jnp.float32
        )
        out_ref[k, :, :orbitals] = (contract(ur, sr) + contract(ui, si)).astype(jnp.bfloat16)
        out_ref[k, :, orbitals:] = (contract(ur, si) - contract(ui, sr)).astype(jnp.bfloat16)


def transform_kernel(scale_by, lattice_count, path_count, pieces, *refs):
    piece_refs = refs[:pieces]
    with_real_ref, with_imag_ref, lattice_ref, path_ref = refs[pieces:]
    orbitals = lattice_ref.shape[-1] // 2
    first = pl.multiple_of(pl.program_id(0) * SUB, SUB)
    blocks = [
        ref[:, pl.ds(first, SUB), :].astype(jnp.float32).reshape(-1, 2 * orbitals) for ref in piece_refs
    ]
    block = jnp.concatenate(blocks, 0).astype(jnp.bfloat16)
    real, imag = block[:, :orbitals], block[:, orbitals:]

    def rows(start, count):
        lo, hi = start * SUB, (start + count) * SUB
        total = jnp.dot(with_real_ref[lo:hi, :], real, preferred_element_type=jnp.float32)
        total += jnp.dot(with_imag_ref[lo:hi, :], imag, preferred_element_type=jnp.float32)
        return total.reshape(count, SUB, orbitals)

    step = math.gcd(lattice_count, 16)
    for start in range(0, lattice_count, step):
        lattice_ref[start : start + step, :, :orbitals] = (rows(start, step) / scale_by).astype(jnp.bfloat16)
        lattice_ref[start : start + step, :, orbitals:] = (
            rows(lattice_count + start, step) / scale_by
        ).astype(jnp.bfloat16)
    values = rows(2 * lattice_count, 4 * path_count)
    path_ref[:, :, :orbitals] = values[:path_count] + values[2 * path_count : 3 * path_count]
    path_ref[:, :, orbitals:] = values[path_count : 2 * path_count] + values[3 * path_count :]


def cos_sin(windings, period):
    angles = windings.astype(jnp.float32) * (2.0 * math.pi / period)
    return jnp.cos(angles), jnp.sin(angles)


def mesh_phases(vectors, coords):
    windings = jnp.mod(jnp.sum(vectors[:, :, None] * coords[:, None, :], 0), MESH)
    cos, sin = cos_sin(windings, MESH)
    return cos.astype(jnp.bfloat16), sin.astype(jnp.bfloat16)


def spread(table):
    count, width = table.shape
    down = lax.broadcasted_iota(jnp.int32, (count * SUB, count), 0) // SUB
    pick = (down == lax.broadcasted_iota(jnp.int32, (count * SUB, count), 1)).astype(jnp.bfloat16)
    along = lax.broadcasted_iota(jnp.int32, (width, width * SUB), 1) // SUB
    place = (along == lax.broadcasted_iota(jnp.int32, (width, width * SUB), 0)).astype(jnp.bfloat16)
    tall = jnp.dot(pick, table, preferred_element_type=jnp.float32).astype(jnp.bfloat16)
    wide = jnp.dot(tall, place, preferred_element_type=jnp.float32)
    lane = lax.broadcasted_iota(jnp.int32, wide.shape, 1) % SUB
    sublane = lax.broadcasted_iota(jnp.int32, wide.shape, 0) % SUB
    return jnp.where(lane == sublane, wide, 0.0).astype(jnp.bfloat16)


def flip(array, axis, mask, size):
    return lax.ppermute(array, axis, [(i, i ^ mask) for i in range(size)])


def local(gauge, energies, kmesh, lattice, degeneracy, path):
    per_device, _, _, orbitals = gauge.shape
    ka_count = lax.axis_size("ka")
    row_count = lax.axis_size("row")
    row = lax.axis_index("row")
    k_total = kmesh.shape[1]
    lattice_count = lattice.shape[1]
    path_count = path.shape[1] // row_count
    local_rows = orbitals // ka_count
    vmem = pl.BlockSpec(memory_space=pltpu.VMEM)

    rotated = pl.pallas_call(
        rotate_kernel,
        out_shape=jax.ShapeDtypeStruct((per_device, orbitals, 2 * orbitals), jnp.bfloat16),
        in_specs=[vmem, vmem],
        out_specs=vmem,
        name="rotate",
    )(gauge, energies)
    arrived = lax.all_to_all(rotated, "ka", split_axis=1, concat_axis=0, tiled=True)

    pieces, offsets = [arrived], [0]
    table = jnp.concatenate([lattice, degeneracy[None, :]], 0)
    mask = row_count // 2
    while mask:
        pieces = pieces + [flip(piece, "row", mask, row_count) for piece in pieces]
        offsets = offsets + [offset ^ mask for offset in offsets]
        table = jnp.concatenate([table, flip(table, "row", mask, row_count)], 1)
        mask //= 2

    by_device = kmesh.reshape(3, ka_count, row_count, per_device)
    coords = jnp.concatenate(
        [
            lax.dynamic_index_in_dim(by_device, row ^ offset, 2, keepdims=False).reshape(3, -1)
            for offset in offsets
        ],
        1,
    )
    cosf, sinf = mesh_phases(lattice, coords)
    vectors_all, counts_all = table[:3], table[3]
    cosf_all, sinf_all = mesh_phases(vectors_all, coords)
    own_path = lax.dynamic_slice_in_dim(path, row * path_count, path_count, 1)
    windings = jnp.mod(jnp.sum(own_path[:, :, None] * vectors_all[:, None, :], 0), PATH_DEN)
    cosp, sinp = cos_sin(windings, PATH_DEN)
    weights = 1.0 / counts_all.astype(jnp.float32)
    factors = jnp.concatenate([cosp * weights, sinp * weights], 0).astype(jnp.bfloat16)
    with_cos = jnp.dot(factors, cosf_all, preferred_element_type=jnp.float32)
    with_sin = jnp.dot(factors, sinf_all, preferred_element_type=jnp.float32)
    mixing_real = (with_cos[:path_count] + with_sin[path_count:]) / k_total
    mixing_imag = (with_cos[path_count:] - with_sin[:path_count]) / k_total
    times_real = jnp.concatenate([mixing_real, mixing_imag], 0)
    times_imag = jnp.concatenate([-mixing_imag, mixing_real], 0)

    def halves(values):
        high = lax.reduce_precision(values, 8, 7)
        return [high.astype(jnp.bfloat16), (values - high).astype(jnp.bfloat16)]

    with_real = spread(jnp.concatenate([cosf, -sinf] + halves(times_real), 0))
    with_imag = spread(jnp.concatenate([sinf, cosf] + halves(times_imag), 0))

    return pl.pallas_call(
        functools.partial(transform_kernel, k_total, lattice_count, path_count, len(pieces)),
        grid=(local_rows // SUB,),
        out_shape=(
            jax.ShapeDtypeStruct((lattice_count, local_rows, 2 * orbitals), jnp.bfloat16),
            jax.ShapeDtypeStruct((path_count, local_rows, 2 * orbitals), jnp.float32),
        ),
        in_specs=[vmem] * (len(pieces) + 2),
        out_specs=(
            pl.BlockSpec((lattice_count, SUB, 2 * orbitals), lambda i: (0, i, 0)),
            pl.BlockSpec((path_count, SUB, 2 * orbitals), lambda i: (0, i, 0)),
        ),
        name="transform",
    )(*pieces, with_real, with_imag)


def solution(mesh):
    return jax.shard_map(
        local,
        mesh=mesh,
        in_specs=(
            P(("ka", "row"), None, None, None),
            P(("ka", "row"), None),
            P(),
            P(None, "row"),
            P("row"),
            P(),
        ),
        out_specs=(P("row", "ka", None), P("row", "ka", None)),
        check_vma=False,
    )
```
